32 devices in a mesh: expert: 4 (over z), tensor: 8 (over y, x, core).
Axes of the slice: x: 2, y: 2, z: 4, core: 2. Of those that a mesh axis runs over, the one named last changes fastest.
Arguments:
- layer_input: bfloat16 [8192, 2048], P('expert'), may hold values from -6 to 6
- cotangent: bfloat16 [8192, 2048], P(('expert', 'tensor')), may hold values from -6 to 6
- lengths: int32 [4, 4], P('expert'), may hold values from 1 to 1024, 2048 in all within a row
- routes: int32 [8192, 8], P(('expert', 'tensor')), may hold values from 0 to 15, all different within a row; in each aligned block of 256 rows (0 to 255, 256 to 511, ...) at most 192 rows name the same one
- attn_gain: float32 [2048], replicated, may hold values from 0.5 to 1.5
- w_qkv: bfloat16 [2048, 3, 2048], P(None, None, 'tensor'), may hold values from -0.125 to 0.125
- q_gain: float32 [128], replicated, may hold values from 0.6 to 5
- k_gain: float32 [128], replicated, may hold values from 0.6 to 5
- w_out: bfloat16 [2048, 2048], P('tensor'), may hold values from -2 to 2
- ffn_gain: float32 [2048], replicated, may hold values from 0.5 to 1.5
- w_router: bfloat16 [2048, 16], replicated, may hold values from -0.125 to 0.125
- w_gate: bfloat16 [16, 2048, 1024], P('expert', None, 'tensor'), may hold values from -0.125 to 0.125
- w_up: bfloat16 [16, 2048, 1024], P('expert', None, 'tensor'), may hold values from -0.125 to 0.125
- w_down: bfloat16 [16, 1024, 2048], P('expert', 'tensor'), may hold values from -6 to 6
Outputs:
- output: bfloat16 [8192, 2048], P(('expert', 'tensor'))
- grad_input: bfloat16 [8192, 2048], P(('expert', 'tensor'))
- grad_attn_gain: float32 [2048], replicated
- grad_w_qkv: float32 [2048, 3, 2048], P(None, None, 'tensor')
- grad_q_gain: float32 [128], replicated
- grad_k_gain: float32 [128], replicated
- grad_w_out: float32 [2048, 2048], P('tensor')
- grad_ffn_gain: float32 [2048], replicated
- grad_w_router: float32 [2048, 16], replicated
- grad_w_gate: float32 [16, 2048, 1024], P('expert', None, 'tensor')
- grad_w_up: float32 [16, 2048, 1024], P('expert', None, 'tensor')
- grad_w_down: float32 [16, 1024, 2048], P('expert', 'tensor')
The draws below stay inside these ranges and needn't reach their ends.
Inputs may be any that keep to these rules, and one draw needn't show every extreme that they name: `routes`: no expert is named by more than 192 of the 256 rows of one device (aligned blocks of rows); in every draw some expert is named 192 times in some block. `lengths`: each row sums to 2048; its longest sequence has exactly 1024 tokens.
All inputs are finite; a program needn't handle non-finite values.
Results may differ from the reference program's by a relative error of at most 0.024.
The reference program's roundings to bfloat16 on the way count: a program that leaves them out, or rounds other values in their place, can miss the bound.
Values may be sent and summed in bfloat16 or wider, within the bound.
A program may use at most 384 MiB of HBM per device.

```python
import math
from functools import partial
import jax
import jax.numpy as jnp
import numpy as np
from jax import lax

D = 2048
HEADS = 16
HEAD_DIM = 128
FE = 1024
TOPK = 8
TOK_DEV = 256
SEQS = 4
GROUP = 2048
TOKENS = 8192
E = 16
CAP = 192
SEQ_MAX = 1024
N_EXPERT = 4
N_TENSOR = 8


def gain_draw(seed_key):
    return jnp.exp(jax.random.uniform(seed_key, (HEAD_DIM,), jnp.float32, -0.5, 0.5))


def draw_q_gain(key, part):
    return gain_draw(jax.random.fold_in(key, 11))


def draw_k_gain(key, part):
    return gain_draw(jax.random.fold_in(key, 12))


def block_scale(own_key, extent, split, least, high):
    factor_of, own = 1.0, jax.random.fold_in(own_key, 6)
    for dim, shards_of in split:
        draws = jnp.exp(jax.random.uniform(jax.random.fold_in(own, dim), (shards_of,), jnp.float32, least / len(split), high / len(split)))
        factor_of = factor_of * jnp.repeat(draws, extent[dim] // shards_of).reshape([-1 if axis == dim else 1 for axis in range(len(extent))])
    return factor_of


def length_profile(number_of, total, bound, slope):
    loads = [(1 << 20) // math.isqrt(standing ** slope) + 1 for standing in range(2, number_of + 1)]
    rest, given = total - bound - (number_of - 1), [1] * (number_of - 1)
    while rest > 0:
        movable = [i for i in range(number_of - 1) if given[i] < bound]
        mass, left = sum([loads[i] for i in movable]), rest
        for i in movable:
            more = min(bound - given[i], max(1, left * loads[i] // mass), rest)
            given[i] = given[i] + more
            rest = rest - more
    return np.array([bound] + given)


def ragged_sizes(stream_key, count, total, bound, lean):
    if count == 2:
        one = jax.random.randint(stream_key, (), max(1, total - bound), min(bound, total - 1) + 1)
        return jnp.stack([one, total - one])
    sizes = jnp.asarray(length_profile(count, total, bound, lean), jnp.int32)
    couples = (count - 1) // 2
    source_of, taker = sizes[1:1 + 2 * couples:2], sizes[2:2 + 2 * couples:2]
    room = jnp.minimum(source_of - 1, bound - taker)
    passed = jax.random.randint(jax.random.fold_in(stream_key, 1), (couples,), 0, 1 << 20) % (room + 1)
    sizes = sizes.at[1:1 + 2 * couples:2].set(source_of - passed).at[2:2 + 2 * couples:2].set(taker + passed)
    return sizes[jax.random.permutation(jax.random.fold_in(stream_key, 2), count)]


def assign_block(own_key, own, number, rows, amount, top, most, skew):
    sequence = jax.random.permutation(own_key, amount)
    crowded, common = load_shares(amount, rows * top, most, skew, True), load_shares(amount, rows * top, most, skew, False)
    places = jnp.arange(amount)

    def named(tallies, rotation):
        used = int((tallies > 0).sum())
        fixed = max(1, used // 4)
        passed = fixed + (places - fixed + rotation * (used - fixed)) % max(1, amount - fixed)
        return jnp.zeros((amount,), jnp.int32).at[sequence[jnp.where(places < fixed, places, passed)]].set(jnp.asarray(tallies, jnp.int32))

    tallies = jnp.where(number % 4 == 0, named(crowded, number // 4), named(common, number - number // 4 - 1))
    mixed = jax.random.permutation(jax.random.fold_in(own, 3), amount)
    donor, sink = mixed[0:amount // 2 * 2:2], mixed[1:amount // 2 * 2:2]
    margin = jnp.minimum(tallies[donor] - 1, most - tallies[sink]) // 2
    margin = jnp.where((donor == sequence[0]) | (sink == sequence[0]) | (tallies[sink] == 0), 0, jnp.maximum(margin, 0))
    passed = jax.random.randint(jax.random.fold_in(own, 4), (amount // 2,), 0, 1 << 20) % (margin + 1)
    tallies = tallies.at[donor].add(-passed).at[sink].add(passed)
    items = jnp.searchsorted(jnp.cumsum(tallies), jnp.arange(rows * top), side="right").astype(jnp.int32)
    listing = items.reshape(top, rows).T
    listing = listing[jax.random.permutation(jax.random.fold_in(own, 1), rows)]
    rotation = jax.random.randint(jax.random.fold_in(own, 2), (rows, 1), 0, top)
    return jnp.take_along_axis(listing, (jnp.arange(top)[None, :] + rotation) % top, axis=1)


def load_shares(amount, total, bound, skew, full):
    loads = [(1 << 20) // math.isqrt(rank ** skew) + 1 for rank in range(1, amount + 1)]
    largest = bound if full else min(bound, max(-(-total // amount), total * loads[0] // sum(loads)))
    least = 1 if total - largest >= amount - 1 else 0
    counts, surplus = [largest] + [least] * (amount - 1), total - largest - least * (amount - 1)
    while surplus > 0:
        movable = [i for i in range(1, amount) if counts[i] < largest] or [i for i in range(1, amount) if counts[i] < bound]
        mass, remaining = sum([loads[i] for i in movable]), surplus
        for i in movable:
            addition = min(bound - counts[i], max(1, remaining * loads[i] // mass), surplus)
            counts[i] = counts[i] + addition
            surplus = surplus - addition
    return np.array(counts)


def noise(rng, shape, deviation, limit, pieces=(), kind=jnp.bfloat16):
    result = deviation * jax.random.normal(rng, shape, jnp.float32)
    if pieces:
        result = result * block_scale(rng, shape, pieces, -0.22, 0.18)
    return jnp.clip(result, -limit, limit).astype(kind)


def setup_inputs(seed: int = 0) -> dict:
    key_list = jax.random.split(jax.random.key(seed), 15)
    layer_input = noise(key_list[0], (TOKENS, D), 1.0, 6.0, ((0, 4),))
    cotangent = noise(key_list[1], (TOKENS, D), 1.0, 6.0, ((0, 32),))
    lengths = jax.vmap(lambda own: ragged_sizes(own, SEQS, GROUP, SEQ_MAX, 2))(jax.random.split(key_list[2], N_EXPERT)).reshape((N_EXPERT, SEQS)).astype(jnp.int32)
    routes_keys = jax.random.split(jax.random.fold_in(key_list[3], 1), TOKENS // TOK_DEV)
    routes_turns = jax.random.permutation(jax.random.fold_in(key_list[3], 3), TOKENS // TOK_DEV)
    routes = jax.vmap(lambda own, number: assign_block(jax.random.fold_in(key_list[3], 2), own, number, TOK_DEV, E, TOPK, CAP, 2))(routes_keys, routes_turns).reshape((TOKENS, TOPK))
    attn_gain = jnp.clip(1.0 + 0.1 * jax.random.normal(key_list[4], (D,), jnp.float32), 0.5, 1.5)
    w_qkv = noise(key_list[5], (D, 3, HEADS * HEAD_DIM), D ** -0.5, 0.125, ((2, 8),))
    q_gain = draw_q_gain(jax.random.fold_in(key_list[14], 71), 0)
    k_gain = draw_k_gain(jax.random.fold_in(key_list[14], 71), 0)
    w_out = noise(key_list[8], (HEADS * HEAD_DIM, D), (max(1, HEADS * HEAD_DIM // 256)) ** -0.5, 2.0, ((0, 8),))
    ffn_gain = jnp.clip(1.0 + 0.1 * jax.random.normal(key_list[9], (D,), jnp.float32), 0.5, 1.5)
    w_router = noise(key_list[10], (D, E), D ** -0.5, 0.125)
    w_gate = noise(key_list[11], (E, D, FE), D ** -0.5, 0.125, ((0, 4), (2, 8)))
    w_up = noise(key_list[12], (E, D, FE), D ** -0.5, 0.125, ((0, 4), (2, 8)))
    w_down = noise(key_list[13], (E, FE, D), (max(1, FE // 1024)) ** -0.5, 6.0, ((0, 4), (1, 8)))
    return dict(layer_input=layer_input, cotangent=cotangent, lengths=lengths, routes=routes, attn_gain=attn_gain, w_qkv=w_qkv, q_gain=q_gain, k_gain=k_gain, w_out=w_out, ffn_gain=ffn_gain, w_router=w_router, w_gate=w_gate, w_up=w_up, w_down=w_down)


@jax.custom_vjp
def low(v):
    return lax.optimization_barrier(v.astype(jnp.bfloat16)).astype(jnp.float32)

@jax.custom_vjp
def low_back(v):
    return v

def low_keep(v):
    return (low(v), None)

def low_pass(kept, grad):
    return (grad,)

def back_keep(v):
    return (v, None)

def back_low(kept, grad):
    return (low(grad),)
low.defvjp(low_keep, low_pass)
low_back.defvjp(back_keep, back_low)
NORM_EPS = 1e-06
ROPE_BASE = 50000.0
HIGHEST = lax.Precision.HIGHEST

def rms_scale(values):
    return lax.rsqrt(lax.optimization_barrier(jnp.mean(values * values, axis=-1, keepdims=True)) + NORM_EPS)

def positions_of(seq_lengths, row_count):
    seq_ends = jnp.cumsum(seq_lengths).astype(jnp.int32)
    starts = (seq_ends - seq_lengths).astype(jnp.int32)
    row_index = jnp.arange(row_count, dtype=jnp.int32)
    segment = lax.optimization_barrier(jnp.sum((row_index[:, None] >= seq_ends[None, :]).astype(jnp.int32), axis=1)).astype(jnp.int32)
    picked = segment[:, None] == jnp.arange(seq_lengths.shape[0], dtype=jnp.int32)[None, :]
    offsets = lax.optimization_barrier(jnp.sum(jnp.where(picked, starts[None, :], 0), axis=1)).astype(jnp.int32)
    return (segment, (row_index - offsets).astype(jnp.int32))

def rotate(values, position):
    half_width = values.shape[-1] // 2
    frequency = jnp.exp(jnp.arange(half_width, dtype=jnp.float32) * (-2.0 * math.log(ROPE_BASE) / values.shape[-1]))
    angle = position.astype(jnp.float32)[:, None] * frequency[None, :]
    cosine = jnp.cos(angle)[:, None, :]
    sine_part = jnp.sin(angle)[:, None, :]
    first_half = values[..., :half_width]
    second = values[..., half_width:]
    return jnp.concatenate([first_half * cosine - second * sine_part, second * cosine + first_half * sine_part], axis=-1)

def shape_heads(qkv_proj, q_gain, k_gain, position):
    query_rows = qkv_proj[:, 0]
    key_rows = qkv_proj[:, 1]
    value_rows = qkv_proj[:, 2]
    query_rows = rotate(query_rows * rms_scale(query_rows) * q_gain, position)
    key_rows = rotate(key_rows * rms_scale(key_rows) * k_gain, position)
    return (query_rows, key_rows, value_rows)

def attend_group(group_item):
    query_rows, key_rows, value_rows, segment = group_item
    row_count, head_count, head_width = query_rows.shape
    block_rows = min(512, row_count)
    score_scale = 1.0 / math.sqrt(head_width)

    def one_block(block_item):
        query_block, segment_block = block_item
        scores = low_back(jnp.einsum('qhd,khd->hqk', query_block, key_rows, precision=HIGHEST) * score_scale)
        same_seq = (segment_block[:, None] == segment[None, :])[None]
        scores = jnp.where(same_seq, scores, -1e+30)
        weights = low(jax.nn.softmax(scores, axis=-1))
        return jnp.einsum('hqk,khd->qhd', weights, value_rows, precision=HIGHEST)
    blocks = (query_rows.reshape(row_count // block_rows, block_rows, head_count, head_width), segment.reshape(row_count // block_rows, block_rows))
    mixed_out = lax.map(jax.checkpoint(one_block), blocks)
    return mixed_out.reshape(row_count, head_count, head_width)

def expert_part(rows_index, gate_weight, up_weight, down_weight, padded_in, padded_gate):
    token_index = rows_index // TOPK
    expert_rows = low_back(padded_in[token_index])
    gate_pre = low_back(jnp.dot(expert_rows, gate_weight, precision=HIGHEST))
    up_pre = low_back(jnp.dot(expert_rows, up_weight, precision=HIGHEST))
    hidden = low(jax.nn.silu(gate_pre) * up_pre)
    expert_out = low(low_back(jnp.dot(hidden, down_weight, precision=HIGHEST)))
    return jnp.zeros(padded_in.shape, padded_in.dtype).at[token_index].add(padded_gate[rows_index][:, None] * expert_out)

def reference(layer_input, cotangent, lengths, routes, attn_gain, w_qkv, q_gain, k_gain, w_out, ffn_gain, w_router, w_gate, w_up, w_down):
    group_rows = TOK_DEV * N_TENSOR
    token_count = layer_input.shape[0]
    segments, positions = jax.vmap(partial(positions_of, row_count=group_rows))(lengths)
    position = positions.reshape(-1)
    flat_routes = routes.reshape(-1).astype(jnp.int32)
    row_total = flat_routes.shape[0]
    rows_dev = TOK_DEV * TOPK
    devices = N_EXPERT * N_TENSOR
    expert_hits = (flat_routes.reshape(devices, rows_dev)[:, :, None] == jnp.arange(E, dtype=jnp.int32)[None, None, :]).astype(jnp.int32)
    slot_index = lax.optimization_barrier(jnp.sum(expert_hits * (jnp.cumsum(expert_hits, axis=1) - 1), axis=2)).astype(jnp.int32).reshape(-1)
    device_index = (jnp.arange(row_total, dtype=jnp.int32) // rows_dev).astype(jnp.int32)
    slot_table = jnp.full((E, devices, CAP), row_total, jnp.int32).at[flat_routes, device_index, slot_index].set(jnp.arange(row_total, dtype=jnp.int32)).reshape(E, devices * CAP)

    def forward(input_full, gain_one, qkv_weight, gain_q, gain_k, out_weight, gain_two, router_weight, gate_weights, up_weights, down_weights):
        scale_one = rms_scale(input_full)
        normed = low(input_full * scale_one * gain_one)
        qkv_proj = low_back(jnp.dot(normed, qkv_weight.reshape(D, 3 * HEADS * HEAD_DIM), precision=HIGHEST))
        qkv_proj = qkv_proj.reshape(token_count, 3, HEADS, HEAD_DIM)
        query_rows, key_rows, value_rows = shape_heads(qkv_proj, gain_q, gain_k, position)
        grouped = (low(query_rows).reshape(N_EXPERT, group_rows, HEADS, HEAD_DIM), low(key_rows).reshape(N_EXPERT, group_rows, HEADS, HEAD_DIM), low(value_rows).reshape(N_EXPERT, group_rows, HEADS, HEAD_DIM), segments)
        mixed_out = lax.map(jax.checkpoint(attend_group), grouped).reshape(token_count, HEADS * HEAD_DIM)
        mixed_out = low(low_back(mixed_out))
        residual = input_full + low_back(jnp.dot(mixed_out, out_weight, precision=HIGHEST))
        scale_two = rms_scale(residual)
        ffn_in = low(residual * scale_two * gain_two)
        logits = low_back(jnp.dot(ffn_in, router_weight, precision=HIGHEST))
        probabilities = jax.nn.softmax(logits, axis=-1)
        gates = jnp.take_along_axis(probabilities, routes, axis=1)
        padded_in = jnp.concatenate([ffn_in, jnp.zeros((1, D), ffn_in.dtype)], axis=0)
        padded_gate = jnp.concatenate([gates.reshape(-1), jnp.zeros((1,), gates.dtype)], axis=0)
        expert_step = jax.checkpoint(expert_part)

        def scan_step(running, scan_item):
            rows_index, gate_weight, up_weight, down_weight = scan_item
            return (running + expert_step(rows_index, gate_weight, up_weight, down_weight, padded_in, padded_gate), None)
        mixture, unused = lax.scan(scan_step, jnp.zeros((token_count + 1, D), input_full.dtype), (slot_table, gate_weights, up_weights, down_weights))
        return residual + mixture[:token_count]
    primals = (layer_input.astype(jnp.float32), attn_gain, w_qkv.astype(jnp.float32), q_gain, k_gain, w_out.astype(jnp.float32), ffn_gain, w_router.astype(jnp.float32), w_gate.astype(jnp.float32), w_up.astype(jnp.float32), w_down.astype(jnp.float32))
    output, pullback = jax.vjp(forward, *primals)
    gradients = pullback(cotangent.astype(jnp.float32))
    return (output.astype(jnp.bfloat16), gradients[0].astype(jnp.bfloat16), gradients[1], gradients[2], gradients[3], gradients[4], gradients[5], gradients[6], gradients[7], gradients[8], gradients[9], gradients[10])
```

```python
import functools
import math

import jax
import jax.numpy as jnp
from jax import lax
from jax.experimental import pallas as pl
from jax.experimental.pallas import tpu as pltpu
from jax.sharding import PartitionSpec as P

NORM_EPS = 1e-06
ROPE_BASE = 50000.0
F32 = jnp.float32
BF16 = jnp.bfloat16
NT = (((1,), (1,)), ((), ()))
TN = (((0,), (0,)), ((), ()))
CORE, NEAR, FAR = 1, 2, 4
VMEM_LIMIT = 60 * 1024 * 1024


def params(**kw):
    return pltpu.CompilerParams(vmem_limit_bytes=VMEM_LIMIT, **kw)


def cost(flops, nbytes, trans=0):
    return pl.CostEstimate(flops=int(flops), bytes_accessed=int(nbytes), transcendentals=int(trans))


def full(shape):
    return pl.BlockSpec(shape, lambda *_: (0,) * len(shape))


def rms_scale(values):
    return lax.rsqrt(jnp.mean(values * values, axis=-1, keepdims=True) + NORM_EPS)


def project_kernel(x, gain, w, cos, sin, q_gain, k_gain, normed, q, k, v, raw, *, heads, width):
    xf = x[...].astype(F32)
    low = (xf * rms_scale(xf) * gain[...]).astype(BF16)
    normed[...] = low
    proj = jnp.dot(low, w[...], preferred_element_type=F32)
    span = heads * width
    raw[...] = proj[:, : 2 * span]
    v[...] = proj[:, 2 * span :].astype(BF16)
    c, s = cos[...], sin[...]
    for part, (out, head_gain) in enumerate(((q, q_gain), (k, k_gain))):
        for h in range(heads):
            u = proj[:, part * span + h * width : part * span + (h + 1) * width]
            u = u * rms_scale(u) * head_gain[...]
            out[:, h * width : (h + 1) * width] = (
                u * c + pltpu.roll(u, width // 2, 1) * s
            ).astype(BF16)


def project(x, gain, w, cos, sin, q_gain, k_gain, heads, width):
    rows, depth = x.shape
    span = heads * width
    blk = min(256, rows)
    row = lambda n: pl.BlockSpec((blk, n), lambda i: (i, 0))
    return pl.pallas_call(
        functools.partial(project_kernel, heads=heads, width=width),
        grid=(rows // blk,),
        in_specs=[row(depth), full((1, depth)), full(w.shape), row(width), row(width), full((1, width)), full((1, width))],
        out_specs=[row(depth), row(span), row(span), row(span), row(2 * span)],
        out_shape=[
            jax.ShapeDtypeStruct((rows, depth), BF16),
            jax.ShapeDtypeStruct((rows, span), BF16),
            jax.ShapeDtypeStruct((rows, span), BF16),
            jax.ShapeDtypeStruct((rows, span), BF16),
            jax.ShapeDtypeStruct((rows, 2 * span), F32),
        ],
        compiler_params=params(),
        cost_estimate=cost(2 * rows * depth * 3 * span, rows * depth * 4 + w.size * 2 + rows * span * 14),
        name="project",
    )(x, gain[None], w, cos, sin, q_gain[None], k_gain[None])


def attend_kernel(lo, hi, seg_col, seg_row, q, k, v, out, lse, s_sc, *, scale, blk):
    i = pl.program_id(1)
    first, last = lo[i], hi[i]
    qb, sr = q[...], seg_row[...]

    def at(j):
        return pl.ds(pl.multiple_of(j * blk, blk), blk)

    def scores(j, peak):
        s = lax.dot_general(k[at(j), :], qb, NT, preferred_element_type=F32) * scale
        s = jnp.where(seg_col[at(j), :] == sr, s, -1e30)
        s_sc[at(j), :] = s
        return jnp.maximum(peak, jnp.max(s, axis=0, keepdims=True))

    peak = lax.fori_loop(first, last, scores, jnp.full((1, blk), -1e30, F32))

    def weights(j, total):
        e = jnp.exp(s_sc[at(j), :] - peak)
        s_sc[at(j), :] = e
        return total + jnp.sum(e, axis=0, keepdims=True)

    total = lax.fori_loop(first, last, weights, jnp.zeros((1, blk), F32))
    inv = 1.0 / total

    def mix(j, acc):
        p = (s_sc[at(j), :] * inv).astype(BF16)
        return acc + lax.dot_general(v[at(j), :], p, TN, preferred_element_type=F32)

    acc = lax.fori_loop(first, last, mix, jnp.zeros((v.shape[1], blk), F32))
    out[...] = acc.T.astype(BF16)
    lse[0] = peak + jnp.log(total)


def attend(q, k, v, seg, lo, hi, heads, width, scale):
    rows = q.shape[0]
    blk = min(256, rows)
    head = pl.BlockSpec((rows, width), lambda h, i, *_: (0, h))
    tile = pl.BlockSpec((blk, width), lambda h, i, *_: (i, h))
    return pl.pallas_call(
        functools.partial(attend_kernel, scale=scale, blk=blk),
        grid_spec=pltpu.PrefetchScalarGridSpec(
            num_scalar_prefetch=2,
            grid=(heads, rows // blk),
            in_specs=[full((rows, 1)), pl.BlockSpec((1, blk), lambda h, i, *_: (0, i)), tile, head, head],
            out_specs=[tile, pl.BlockSpec((1, 1, blk), lambda h, i, *_: (h, 0, i))],
            scratch_shapes=[pltpu.VMEM((rows, blk), F32)],
        ),
        out_shape=[
            jax.ShapeDtypeStruct((rows, heads * width), BF16),
            jax.ShapeDtypeStruct((heads, 1, rows), F32),
        ],
        compiler_params=params(),
        cost_estimate=cost(2 * heads * rows * rows * width, heads * rows * width * 8, heads * rows * rows // 2),
        name="attend",
    )(lo, hi, seg[:, None], seg[None, :], q, k, v)


def attend_back_kernel(lo, hi, seg_col, seg_row, lse, q, k, v, g, dq, dk, dv, p_sc, d_sc, *, scale, blk):
    i = pl.program_id(1)
    first, last = lo[i], hi[i]
    qb, gb, sr, total = q[...], g[...], seg_row[...], lse[0]

    @pl.when(i == 0)
    def _():
        dk[...] = jnp.zeros_like(dk)
        dv[...] = jnp.zeros_like(dv)

    def at(j):
        return pl.ds(pl.multiple_of(j * blk, blk), blk)

    def forward(j, delta):
        s = lax.dot_general(k[at(j), :], qb, NT, preferred_element_type=F32) * scale
        s = jnp.where(seg_col[at(j), :] == sr, s, -1e30)
        p = jnp.exp(s - total)
        d = lax.dot_general(v[at(j), :], gb, NT, preferred_element_type=F32)
        p_sc[at(j), :] = p
        d_sc[at(j), :] = d
        return delta + jnp.sum(p * d, axis=0, keepdims=True)

    delta = lax.fori_loop(first, last, forward, jnp.zeros((1, blk), F32))

    def backward(j, acc):
        p = p_sc[at(j), :]
        ds = (p * (d_sc[at(j), :] - delta)).astype(BF16)
        dv[at(j), :] += jnp.dot(p.astype(BF16), gb, preferred_element_type=F32)
        dk[at(j), :] += jnp.dot(ds, qb, preferred_element_type=F32) * scale
        return acc + lax.dot_general(k[at(j), :], ds, TN, preferred_element_type=F32)

    acc = lax.fori_loop(first, last, backward, jnp.zeros((q.shape[1], blk), F32))
    dq[...] = acc.T * scale


def attend_back(q, k, v, g, lse, seg, lo, hi, heads, width, scale):
    rows = q.shape[0]
    blk = min(256, rows)
    head = pl.BlockSpec((rows, width), lambda h, i, *_: (0, h))
    tile = pl.BlockSpec((blk, width), lambda h, i, *_: (i, h))
    shape = jax.ShapeDtypeStruct((rows, heads * width), F32)
    return pl.pallas_call(
        functools.partial(attend_back_kernel, scale=scale, blk=blk),
        grid_spec=pltpu.PrefetchScalarGridSpec(
            num_scalar_prefetch=2,
            grid=(heads, rows // blk),
            in_specs=[
                full((rows, 1)),
                pl.BlockSpec((1, blk), lambda h, i, *_: (0, i)),
                pl.BlockSpec((1, 1, blk), lambda h, i, *_: (h, 0, i)),
                tile, head, head, tile,
            ],
            out_specs=[tile, head, head],
            scratch_shapes=[pltpu.VMEM((rows, blk), F32)] * 2,
        ),
        out_shape=[shape] * 3,
        compiler_params=params(),
        cost_estimate=cost(5 * heads * rows * rows * width, heads * rows * width * 20, heads * rows * rows // 2),
        name="attend_back",
    )(lo, hi, seg[:, None], seg[None, :], lse, q, k, v, g)


def shape_back_kernel(dq, dk, dv, raw, cos, sin, q_gain, k_gain, out, gq, gk, *, heads, width):
    span = heads * width
    c, s = cos[...], sin[...]

    @pl.when(pl.program_id(0) == 0)
    def _():
        gq[...] = jnp.zeros_like(gq)
        gk[...] = jnp.zeros_like(gk)

    for part, (grad, head_gain, gain_sum) in enumerate(((dq, q_gain, gq), (dk, k_gain, gk))):
        for h in range(heads):
            y = grad[:, h * width : (h + 1) * width]
            x = raw[:, part * span + h * width : part * span + (h + 1) * width]
            r = rms_scale(x)
            du = y * c - pltpu.roll(y, width // 2, 1) * s
            gain_sum[...] += jnp.sum(du * x * r, axis=0, keepdims=True)
            scaled = du * head_gain[...]
            back = r * (scaled - x * r * r * jnp.mean(scaled * x, axis=-1, keepdims=True))
            out[:, part * span + h * width : part * span + (h + 1) * width] = back.astype(BF16)
    out[:, 2 * span :] = dv[...].astype(BF16)


def shape_back(dq, dk, dv, raw, cos, sin, q_gain, k_gain, heads, width):
    rows, span = dq.shape
    blk = min(256, rows)
    row = lambda n: pl.BlockSpec((blk, n), lambda i: (i, 0))
    return pl.pallas_call(
        functools.partial(shape_back_kernel, heads=heads, width=width),
        grid=(rows // blk,),
        in_specs=[row(span), row(span), row(span), row(2 * span), row(width), row(width), full((1, width)), full((1, width))],
        out_specs=[row(3 * span), full((1, width)), full((1, width))],
        out_shape=[
            jax.ShapeDtypeStruct((rows, 3 * span), BF16),
            jax.ShapeDtypeStruct((1, width), F32),
            jax.ShapeDtypeStruct((1, width), F32),
        ],
        compiler_params=params(),
        cost_estimate=cost(rows * span * 60, rows * span * 30),
        name="shape_back",
    )(dq, dk, dv, raw, cos, sin, q_gain[None], k_gain[None])


def expert_kernel(*refs, pieces, unit, expert, first):
    x, g, gates = refs[:3]
    gu_hbm, d_hbm = refs[3 : 3 + pieces], refs[3 + pieces : 3 + 2 * pieces]
    outs = refs[3 + 2 * pieces :]
    hg, hg_t, dgu, dgates = outs[:4]
    x_t = outs[4] if first else None
    gu_w, d_w, sems = outs[-3:]

    @pl.when(pl.program_id(0) == 0)
    def _():
        copies = []
        for s in range(pieces):
            copies.append(pltpu.make_async_copy(gu_hbm[s], gu_w.at[:, s * 2 * unit : (s + 1) * 2 * unit], sems.at[2 * s]))
            copies.append(pltpu.make_async_copy(d_hbm[s], d_w.at[s * unit : (s + 1) * unit, :], sems.at[2 * s + 1]))
        for copy in copies:
            copy.start()
        for copy in copies:
            copy.wait()

    xb = x[...]
    gate = gates[:, expert : expert + 1]
    both = jnp.dot(xb, gu_w[...], preferred_element_type=F32)
    back = lax.dot_general(g[...], d_w[...], NT, preferred_element_type=F32)
    acc = jnp.zeros((xb.shape[0], unit), F32)
    for s in range(pieces):
        pre = both[:, 2 * s * unit : (2 * s + 1) * unit]
        up = both[:, (2 * s + 1) * unit : (2 * s + 2) * unit]
        t = back[:, s * unit : (s + 1) * unit]
        sig = 1.0 / (1.0 + jnp.exp(-pre))
        act = pre * sig
        hid = (act * up).astype(BF16).astype(F32)
        acc = acc + hid * t
        dh = gate * t
        dgu[:, 2 * s * unit : (2 * s + 1) * unit] = (dh * up * sig * (1.0 + pre * (1.0 - sig))).astype(BF16)
        dgu[:, (2 * s + 1) * unit : (2 * s + 2) * unit] = (dh * act).astype(BF16)
        low = (gate * hid).astype(BF16)
        hg[:, s * unit : (s + 1) * unit] = low
        hg_t[s * unit : (s + 1) * unit, :] = low.T
    dgates[...] = jnp.sum(acc, axis=1, keepdims=True)
    if first:
        x_t[...] = xb.T


def expert_forward(x, g, gates, gu, d, expert, first):
    rows, depth = x.shape
    pieces, unit = len(gu), d[0].shape[0]
    hidden = pieces * unit
    blk = min(256, rows)
    row = lambda n: pl.BlockSpec((blk, n), lambda i: (i, 0))
    any_spec = pl.BlockSpec(memory_space=pl.ANY)
    out_specs = [row(hidden), pl.BlockSpec((hidden, blk), lambda i: (0, i)), row(2 * hidden), row(1)]
    out_shape = [
        jax.ShapeDtypeStruct((rows, hidden), BF16),
        jax.ShapeDtypeStruct((hidden, rows), BF16),
        jax.ShapeDtypeStruct((rows, 2 * hidden), BF16),
        jax.ShapeDtypeStruct((rows, 1), F32),
    ]
    if first:
        out_specs.append(pl.BlockSpec((depth, blk), lambda i: (0, i)))
        out_shape.append(jax.ShapeDtypeStruct((depth, rows), BF16))
    return pl.pallas_call(
        functools.partial(expert_kernel, pieces=pieces, unit=unit, expert=expert, first=first),
        grid=(rows // blk,),
        in_specs=[row(depth), row(depth), row(gates.shape[1])] + [any_spec] * (2 * pieces),
        out_specs=out_specs,
        out_shape=out_shape,
        scratch_shapes=[
            pltpu.VMEM((depth, 2 * hidden), BF16),
            pltpu.VMEM((hidden, depth), BF16),
            pltpu.SemaphoreType.DMA((2 * pieces,)),
        ],
        compiler_params=params(),
        cost_estimate=cost(6 * rows * depth * hidden, rows * depth * 4 + hidden * depth * 6 + rows * hidden * 8),
        name=f"expert_forward_{expert}",
    )(x, g, gates, *gu, *d)


def input_back_kernel(*refs, experts, pieces):
    grads, weights, out = refs[:experts], refs[experts:-1], refs[-1]
    left = jnp.concatenate([r[...] for r in grads], axis=1)
    right = jnp.concatenate([r[...] for r in weights], axis=1)
    out[...] = lax.dot_general(left, right, NT, preferred_element_type=F32).astype(BF16)


def input_back(grads, weights, chunk, rows):
    experts, pieces = len(grads), len(weights[0])
    depth, wide = weights[0][0].shape
    cols = min(512, depth)
    return pl.pallas_call(
        functools.partial(input_back_kernel, experts=experts, pieces=pieces),
        grid=(depth // cols,),
        in_specs=[pl.BlockSpec((rows, grads[0].shape[1]), lambda j: (chunk, 0))] * experts
        + [pl.BlockSpec((cols, wide), lambda j: (j, 0))] * (experts * pieces),
        out_specs=pl.BlockSpec((rows, cols), lambda j: (0, j)),
        out_shape=jax.ShapeDtypeStruct((rows, depth), BF16),
        compiler_params=params(),
        cost_estimate=cost(2 * rows * depth * experts * pieces * wide, experts * pieces * wide * (depth + rows) * 2 + rows * depth * 2),
        name=f"input_back_{chunk}",
    )(*grads, *[w for per in weights for w in per])


def output_sum_kernel(*refs, experts):
    hidden, weights, out = refs[:experts], refs[experts:-1], refs[-1]
    left = jnp.concatenate([r[...] for r in hidden], axis=1)
    right = jnp.concatenate([r[...] for r in weights], axis=0)
    out[...] = jnp.dot(left, right, preferred_element_type=F32).astype(BF16)


def output_sum(hidden, weights):
    experts, pieces = len(hidden), len(weights[0])
    rows = hidden[0].shape[0]
    unit, depth = weights[0][0].shape
    cols, blk = min(512, depth), min(512, rows)
    return pl.pallas_call(
        functools.partial(output_sum_kernel, experts=experts),
        grid=(depth // cols, rows // blk),
        in_specs=[pl.BlockSpec((blk, hidden[0].shape[1]), lambda j, i: (i, 0))] * experts
        + [pl.BlockSpec((unit, cols), lambda j, i: (0, j))] * (experts * pieces),
        out_specs=pl.BlockSpec((blk, cols), lambda j, i: (i, j)),
        out_shape=jax.ShapeDtypeStruct((rows, depth), BF16),
        compiler_params=params(),
        cost_estimate=cost(2 * rows * depth * experts * pieces * unit, experts * pieces * unit * (depth + rows) * 2 + rows * depth * 2),
        name="output_sum",
    )(*hidden, *[w for per in weights for w in per])


def weight_back_kernel(x_t, dgu, hg_t, g, *outs, pieces, unit):
    gu = jnp.dot(x_t[...], dgu[...], preferred_element_type=F32).astype(BF16)
    d = jnp.dot(hg_t[...], g[...], preferred_element_type=F32).astype(BF16)
    for s in range(pieces):
        outs[s][...] = gu[:, 2 * s * unit : 2 * (s + 1) * unit]
        outs[pieces + s][...] = d[s * unit : (s + 1) * unit, :]


def weight_back(x_t, dgu, hg_t, g, pieces, expert):
    depth, rows = x_t.shape
    hidden = hg_t.shape[0]
    unit = hidden // pieces
    blk = min(256, depth)
    outs = pl.pallas_call(
        functools.partial(weight_back_kernel, pieces=pieces, unit=unit),
        grid=(depth // blk,),
        in_specs=[
            pl.BlockSpec((blk, rows), lambda i: (i, 0)),
            full(dgu.shape),
            full(hg_t.shape),
            pl.BlockSpec((rows, blk), lambda i: (0, i)),
        ],
        out_specs=[pl.BlockSpec((blk, 2 * unit), lambda i: (i, 0))] * pieces
        + [pl.BlockSpec((unit, blk), lambda i: (0, i))] * pieces,
        out_shape=[jax.ShapeDtypeStruct((depth, 2 * unit), BF16)] * pieces
        + [jax.ShapeDtypeStruct((unit, depth), BF16)] * pieces,
        compiler_params=params(),
        cost_estimate=cost(6 * rows * depth * hidden, rows * depth * 4 + hidden * depth * 6 + rows * hidden * 6),
        name=f"weight_back_{expert}",
    )(x_t, dgu, hg_t, g)
    return list(outs[:pieces]), list(outs[pieces:])


def swap(value, mask):
    size = lax.axis_size("tensor")
    return lax.ppermute(value, "tensor", [(i, i ^ mask) for i in range(size)])


def chain_gather(value):
    size = lax.axis_size("expert")
    here = lax.axis_index("expert")
    ups, downs = [value], [value]
    for k in range(size - 1):
        ups.append(lax.ppermute(ups[-1], "expert", [(i, i + 1) for i in range(k, size - 1)]))
        downs.append(lax.ppermute(downs[-1], "expert", [(i + 1, i) for i in range(size - 1 - k)]))
    return [value] + [jnp.where(here >= s, ups[s], downs[size - s]) for s in range(1, size)]


def send_back(value, step):
    size = lax.axis_size("expert")
    if step == 0:
        return value
    return lax.ppermute(value, "expert", [(i, (i - step) % size) for i in range(size)])


def all_sum(value):
    for axis in ("tensor", "expert"):
        size = lax.axis_size(axis)
        bit = 1
        while bit < size:
            value = value + lax.ppermute(value, axis, [(i, i ^ bit) for i in range(size)])
            bit *= 2
    return value


def chain_sum(value):
    size = lax.axis_size("expert")
    here = lax.axis_index("expert")
    rows, columns = value.shape
    part = rows // size
    low = value.astype(BF16)
    total = lax.dynamic_slice_in_dim(value, here * part, part, 0).astype(BF16).astype(F32)
    for s in range(1, size):
        piece = lax.dynamic_slice_in_dim(low, ((here - s) % size) * part, part, 0)
        total = total + send_back(piece, s).astype(F32)
    total = total.astype(BF16)
    out = jnp.zeros((rows, columns), F32)
    for s, piece in enumerate(chain_gather(total)):
        out = lax.dynamic_update_slice(out, piece.astype(F32), (((here - s) % size) * part, 0))
    return out


def tie(values, after):
    return lax.optimization_barrier((values, after))[0]


def experts_dense(ffn_in, gates_all, grads, w_gate, w_up, w_down, after):
    own, depth = ffn_in.shape
    here = lax.axis_index("expert")
    size = lax.axis_size("expert")
    count, _, unit = w_gate.shape
    gu, down = [], []
    for e in range(count):
        pack = (jnp.concatenate([w_gate[e], w_up[e]], axis=1), w_down[e])
        if e > 0:
            pack = tie(pack, after)
        near = [swap(v, NEAR) for v in pack]
        far = [swap(v, FAR) for v in pack]
        both = [swap(v, FAR) for v in near] if e % 2 == 0 else [swap(v, NEAR) for v in far]
        gu.append([pack[0], near[0], far[0], both[0]])
        down.append([pack[1], near[1], far[1], both[1]])
    rows = []
    for piece in chain_gather(ffn_in):
        rows += [piece, swap(piece, CORE)]
    x = jnp.concatenate(rows, axis=0)
    pair = jnp.stack([gates_all, swap(gates_all, CORE)])
    pair = lax.dynamic_slice_in_dim(jnp.concatenate(chain_gather(pair), axis=0).reshape(2 * size * own, -1), here * count, count, 1)
    hidden, hidden_t, pre_grads, gate_grads, x_t = [], [], [], [], None
    weight_grads = []
    for e in range(count):
        out = expert_forward(x, grads, pair, gu[e], down[e], e, e == 0)
        if e == 0:
            x_t = out[4]
        hidden.append(out[0])
        hidden_t.append(out[1])
        pre_grads.append(out[2])
        gate_grads.append(out[3])
    back = jnp.concatenate(gate_grads, axis=1).reshape(size, 2, own, count)
    back = back[:, 0] + swap(back[:, 1], CORE)
    back = jnp.stack([send_back(back[s], s) for s in range(size)])
    twice = jnp.concatenate([back, back], axis=0)
    by_index = lax.dynamic_slice_in_dim(twice, size - here, size, 0)
    grad_gates = by_index.transpose(1, 0, 2).reshape(own, size * count)

    def to_owner(chunk, s):
        mine = chunk[:own].astype(F32) + swap(chunk[own:], CORE).astype(F32)
        return send_back(mine.astype(BF16), s)

    order = list(range(1, size)) + [0]
    grad_rows = 0.0
    for s in order:
        grad_rows = grad_rows + to_owner(input_back(pre_grads, gu, s, 2 * own), s).astype(F32)
    for e in range(count):
        weight_grads.append(weight_back(x_t, pre_grads[e], hidden_t[e], grads, len(gu[e]), e))
    mixed = output_sum(hidden, down)
    mixture = 0.0
    for s in order:
        mixture = mixture + to_owner(mixed[2 * own * s : 2 * own * (s + 1)], s).astype(F32)
    sums_gu, sums_d = [], []
    for e, (p_gu, p_d) in enumerate(weight_grads):
        first, second = (2, 1) if e % 2 == 0 else (1, 2)
        results = []
        for p in (p_gu, p_d):
            late = (p[second].astype(F32) + swap(p[3], (NEAR, FAR)[first - 1]).astype(F32)).astype(BF16)
            got_first = swap(p[first], (NEAR, FAR)[first - 1])
            got_second = swap(late, (NEAR, FAR)[second - 1])
            results.append(p[0].astype(F32) + got_first.astype(F32) + got_second.astype(F32))
        sums_gu.append(results[0])
        sums_d.append(results[1])
    grad_gate = jnp.stack([v[:, :unit] for v in sums_gu])
    grad_up = jnp.stack([v[:, unit:] for v in sums_gu])
    grad_down = jnp.stack(sums_d)
    return mixture, grad_gates, grad_rows, grad_gate, grad_up, grad_down


def swiglu_back(grad_hidden, gate_pre, up_pre):
    sigmoid = jax.nn.sigmoid(gate_pre)
    grad_gate = grad_hidden * up_pre * sigmoid * (1.0 + gate_pre * (1.0 - sigmoid))
    grad_up = grad_hidden * gate_pre * sigmoid
    return (grad_gate.astype(BF16), grad_up.astype(BF16))


def experts_routed(ffn_in, gate_weights, routes, grad_output, w_gate, w_up, w_down, experts_all, capacity):
    own_rows, model_width = ffn_in.shape
    top_count = routes.shape[1]
    experts_here = w_gate.shape[0]
    senders = lax.axis_size("expert")
    flat_routes = routes.reshape(-1)
    expert_hits = (flat_routes[:, None] == jnp.arange(experts_all, dtype=jnp.int32)[None, :]).astype(jnp.int32)
    slot_index = jnp.sum(expert_hits * (jnp.cumsum(expert_hits, axis=0) - 1), axis=1)
    spread_in = jnp.broadcast_to(ffn_in[:, None, :], (own_rows, top_count, model_width)).reshape(-1, model_width)
    spread_grad = (gate_weights[:, :, None] * grad_output[:, None, :]).astype(BF16).reshape(-1, model_width)
    empty = jnp.zeros((experts_all, capacity, model_width), BF16)
    layout = (senders, experts_here, capacity, model_width)
    exchange = functools.partial(lax.all_to_all, axis_name="expert", split_axis=0, concat_axis=0, tiled=True)
    recv_rows = exchange(empty.at[flat_routes, slot_index].set(spread_in).reshape(layout))
    expert_grad = exchange(empty.at[flat_routes, slot_index].set(spread_grad).reshape(layout))
    gate_full = lax.all_gather(w_gate, "tensor", axis=2, tiled=True)
    up_full = lax.all_gather(w_up, "tensor", axis=2, tiled=True)
    down_full = lax.all_gather(w_down, "tensor", axis=1, tiled=True)
    dot = functools.partial(jnp.einsum, preferred_element_type=F32)
    gate_all = dot("sctd,cdf->sctf", recv_rows, gate_full)
    up_all = dot("sctd,cdf->sctf", recv_rows, up_full)
    hidden_low = (jax.nn.silu(gate_all) * up_all).astype(BF16)
    expert_out = dot("sctf,cfd->sctd", hidden_low, down_full).astype(BF16)
    grad_hidden = dot("sctd,cfd->sctf", expert_grad, down_full)
    grad_gate_pre, grad_up_pre = swiglu_back(grad_hidden, gate_all, up_all)
    whole_down = dot("sctf,sctd->cfd", hidden_low, expert_grad)
    whole_gate = dot("sctd,sctf->cdf", recv_rows, grad_gate_pre)
    whole_up = dot("sctd,sctf->cdf", recv_rows, grad_up_pre)
    grad_inputs = (dot("sctf,cdf->sctd", grad_gate_pre, gate_full) + dot("sctf,cdf->sctd", grad_up_pre, up_full)).astype(BF16)

    def scatter(whole, dim):
        return lax.psum_scatter(whole.astype(BF16), "tensor", scatter_dimension=dim, tiled=True).astype(F32)

    pick_index = flat_routes * capacity + slot_index

    def picked(values):
        return (
            exchange(values).reshape(experts_all * capacity, model_width)[pick_index]
            .reshape(own_rows, top_count, model_width).astype(F32)
        )

    rows_back, grads_back = picked(expert_out), picked(grad_inputs)
    mixture = jnp.sum(gate_weights[:, :, None] * rows_back, axis=1)
    grad_gates = jnp.sum(grad_output[:, None, :] * rows_back, axis=-1)
    return mixture, grad_gates, jnp.sum(grads_back, axis=1), scatter(whole_gate, 2), scatter(whole_up, 2), scatter(whole_down, 1)


def body(
    layer_input, cotangent, lengths, routes, attn_gain, w_qkv, q_gain, k_gain, w_out, ffn_gain, w_router, w_gate, w_up, w_down,
):
    group_rows, model_width = layer_input.shape
    own_rows, top_count = routes.shape
    width = q_gain.shape[0]
    heads = w_qkv.shape[2] // width
    span = heads * width
    experts_all = w_router.shape[1]
    ranks = lax.axis_size("tensor")
    rank = lax.axis_index("tensor")
    capacity = max(2, 3 * own_rows * top_count // (2 * experts_all))
    dense = 2 * own_rows <= 3 * capacity and ranks == 8
    scale = 1.0 / math.sqrt(width)

    if dense:
        grads = []
        for piece in chain_gather(cotangent):
            grads += [piece, swap(piece, CORE)]
        grads = jnp.concatenate(grads, axis=0)
    out_weight = lax.all_gather(w_out, "tensor", axis=0, tiled=True)

    seq_lengths = lengths[0]
    ends = jnp.cumsum(seq_lengths)
    starts = ends - seq_lengths
    index = jnp.arange(group_rows, dtype=jnp.int32)
    segment = jnp.sum((index[:, None] >= ends[None, :]).astype(jnp.int32), axis=1)
    offset = jnp.max(jnp.where(index[:, None] >= starts[None, :], starts[None, :], 0), axis=1)
    position = index - offset
    blk = min(256, group_rows)
    tops = jnp.arange(group_rows // blk, dtype=jnp.int32) * blk
    lo = jnp.max(jnp.where(tops[:, None] >= starts[None, :], starts[None, :], 0), axis=1) // blk
    tails = tops + blk - 1
    hi = jnp.min(jnp.where(tails[:, None] < ends[None, :], ends[None, :], group_rows), axis=1)
    hi = (hi + blk - 1) // blk
    half = width // 2
    frequency = jnp.exp(jnp.arange(half, dtype=F32) * (-2.0 * math.log(ROPE_BASE) / width))
    angle = position.astype(F32)[:, None] * frequency[None, :]
    cosine, sine = jnp.cos(angle), jnp.sin(angle)
    cosine = jnp.concatenate([cosine, cosine], axis=1)
    sine = jnp.concatenate([-sine, sine], axis=1)

    qkv_weight = w_qkv.reshape(model_width, 3 * span)
    normed, q, k, v, raw = project(layer_input, attn_gain, qkv_weight, cosine, sine, q_gain, k_gain, heads, width)
    mixed, lse = attend(q, k, v, segment, lo, hi, heads, width, scale)

    mixed_own = lax.all_to_all(mixed.reshape(ranks, own_rows, span), "tensor", split_axis=0, concat_axis=0, tiled=True)
    mixed_own = mixed_own.transpose(1, 0, 2).reshape(own_rows, ranks * span)
    input_own = lax.dynamic_slice_in_dim(layer_input, rank * own_rows, own_rows, 0).astype(F32)
    scale_own = rms_scale(input_own)
    residual = input_own + jnp.dot(mixed_own, out_weight, preferred_element_type=F32)
    scale_two = rms_scale(residual)
    ffn_in = (residual * scale_two * ffn_gain).astype(BF16)
    logits = jnp.dot(ffn_in, w_router, preferred_element_type=F32)
    probabilities = jax.nn.softmax(logits, axis=-1)
    chosen = routes[:, :, None] == jnp.arange(experts_all, dtype=jnp.int32)[None, None, :]
    grad_output = cotangent.astype(F32)
    if dense:
        any_chosen = jnp.any(chosen, axis=1)
        gates_all = jnp.where(any_chosen, probabilities, 0.0)
        mixture, grad_gates, grad_rows, grad_gate, grad_up, grad_down = experts_dense(
            ffn_in, gates_all, grads, w_gate, w_up, w_down, mixed_own
        )
        grad_probs = jnp.where(any_chosen, grad_gates, 0.0)
    else:
        gate_weights = jnp.sum(jnp.where(chosen, probabilities[:, None, :], 0.0), axis=-1)
        mixture, grad_gates, grad_rows, grad_gate, grad_up, grad_down = experts_routed(
            ffn_in, gate_weights, routes, grad_output, w_gate, w_up, w_down, experts_all, capacity
        )
        grad_probs = jnp.sum(jnp.where(chosen, grad_gates[:, :, None], 0.0), axis=1)
    output = (residual + mixture).astype(BF16)
    grad_logits = (
        probabilities * (grad_probs - jnp.sum(grad_probs * probabilities, axis=-1, keepdims=True))
    ).astype(BF16)
    router_part = lax.dot_general(ffn_in, grad_logits, TN, preferred_element_type=F32)
    grad_ffn = grad_rows + lax.dot_general(grad_logits, w_router, NT, preferred_element_type=F32)
    ffn_gain_part = jnp.sum(grad_ffn * residual * scale_two, axis=0)
    scaled_two = grad_ffn * ffn_gain
    grad_residual = grad_output + scale_two * (
        scaled_two - residual * scale_two * scale_two * jnp.mean(scaled_two * residual, axis=-1, keepdims=True)
    )
    grad_attn = grad_residual.astype(BF16)

    grad_mixed = lax.dot_general(grad_attn, out_weight, NT, preferred_element_type=F32).astype(BF16)
    grad_mixed = grad_mixed.reshape(own_rows, ranks, span).transpose(1, 0, 2)
    grad_mixed = lax.all_to_all(grad_mixed, "tensor", split_axis=0, concat_axis=0, tiled=True).reshape(group_rows, span)
    grad_attn_all = lax.all_gather(grad_attn, "tensor", axis=0, tiled=True)
    out_part = lax.dot_general(mixed, grad_attn_all, TN, preferred_element_type=F32)
    grad_q, grad_k, grad_v = attend_back(q, k, v, grad_mixed, lse, segment, lo, hi, heads, width, scale)
    grad_qkv, q_gain_part, k_gain_part = shape_back(grad_q, grad_k, grad_v, raw, cosine, sine, q_gain, k_gain, heads, width)
    qkv_part = lax.dot_general(normed, grad_qkv, TN, preferred_element_type=F32)
    grad_normed = lax.psum_scatter(
        lax.dot_general(grad_qkv, qkv_weight, NT, preferred_element_type=F32).astype(BF16),
        "tensor", scatter_dimension=0, tiled=True,
    ).astype(F32)
    attn_gain_part = jnp.sum(qkv_weight.astype(F32) * qkv_part, axis=1) / attn_gain
    scaled_one = grad_normed * attn_gain
    grad_input = grad_residual + scale_own * (
        scaled_one - input_own * scale_own * scale_own * jnp.mean(scaled_one * input_own, axis=-1, keepdims=True)
    )
    grad_out_sum = chain_sum(out_part)
    grad_qkv_sum = chain_sum(qkv_part).reshape(w_qkv.shape)
    early = all_sum(jnp.concatenate([router_part.T, ffn_gain_part[None]], axis=0))
    late = all_sum(jnp.concatenate([attn_gain_part[None], jnp.pad(jnp.concatenate([q_gain_part, k_gain_part], axis=1), ((0, 0), (0, model_width - 2 * width)))], axis=0))
    return (
        output,
        grad_input.astype(BF16),
        late[0],
        grad_qkv_sum,
        late[1, :width],
        late[1, width : 2 * width],
        grad_out_sum,
        early[experts_all],
        early[:experts_all].T,
        grad_gate,
        grad_up,
        grad_down,
    )


def solution(mesh):
    in_specs = (
        P("expert", None),
        P(("expert", "tensor"), None),
        P("expert", None),
        P(("expert", "tensor"), None),
        P(),
        P(None, None, "tensor"),
        P(),
        P(),
        P("tensor", None),
        P(),
        P(),
        P("expert", None, "tensor"),
        P("expert", None, "tensor"),
        P("expert", "tensor", None),
    )
    out_specs = (
        P(("expert", "tensor"), None),
        P(("expert", "tensor"), None),
        P(),
        P(None, None, "tensor"),
        P(),
        P(),
        P("tensor", None),
        P(),
        P(),
        P("expert", None, "tensor"),
        P("expert", None, "tensor"),
        P("expert", "tensor", None),
    )
    return jax.shard_map(body, mesh=mesh, in_specs=in_specs, out_specs=out_specs, check_vma=False)
```
